32 devices in a mesh: net: 4 (over y, x), line: 8 (over z, core).
Axes of the slice: x: 2, y: 2, z: 4, core: 2. Of those that a mesh axis runs over, the one named last changes fastest.
Arguments:
- conductance_inverse: float32 [4, 4096, 4096], P('net', 'line'), may hold values from -0.5 to 4.5, as said below
- prior_voltage: float32 [4, 96, 4096], P('net', None, 'line'), may hold values from -6 to 6
- sources: float32 [3, 4, 4096], P(None, 'net', 'line'), may hold values from -6 to 6
- fault_node: int32 [96], replicated, may hold values from 0 to 16383
- fault_conductance: float32 [96], replicated, may hold values from 0.5 to 4
- terminal_node: int32 [4, 3, 4096], P('net', None, 'line'), may hold values from 0 to 4095
- ownership: int32 [4, 4096], P('net', 'line'), may hold values from 0 to 1, as said below
- partner: int32 [4, 4096], P('net', 'line'), may hold values from 0 to 31, as said below
- delay_steps: int32 [4, 4096], P('net', 'line'), may hold values from 1 to 4, as said below
- surge_conductance: float32 [4, 4096], P('net', 'line'), may hold values from 0.2 to 1
- pole_wave: float32 [4, 6, 4096], P('net', None, 'line'), may hold values from 0.2 to 0.95
- residue_wave: float32 [4, 6, 3, 3, 4096], P('net', None, None, None, 'line'), may hold values from -1 to 1
- pole_admit: float32 [4, 6, 4096], P('net', None, 'line'), may hold values from 0.2 to 0.95
- residue_admit: float32 [4, 6, 3, 3, 4096], P('net', None, None, None, 'line'), may hold values from -1 to 1
- wave_state: float32 [4, 6, 3, 96, 4096], P('net', None, None, None, 'line'), may hold values from -4 to 4
- admit_state: float32 [4, 6, 3, 96, 4096], P('net', None, None, None, 'line'), may hold values from -4 to 4
- wave_history: float32 [4, 4, 3, 96, 4096], P('net', None, None, None, 'line'), may hold values from -6 to 6
Outputs:
- final_voltage: float32 [4, 96, 4096], P('net', None, 'line')
- end_current: float32 [4, 3, 96, 4096], P('net', None, None, 'line')
The draws below stay inside these ranges and needn't reach their ends.
Inputs may be any that keep to these rules, and one draw needn't show every extreme that they name: `conductance_inverse`: each block is exactly symmetric. `ownership`: A slot is live exactly when the slot of the same number j % 512 at its partner owner is live; the number of live slots differs from owner to owner. The far end of slot j lies in the slot of the same number j % 512 at the partner owner, the partner of that slot is the first owner again, never the owner itself, and at most 17 live slots of one owner have the same partner; this many occur. `delay_steps`: equal at both ends of a line.
All inputs are finite; a program needn't handle non-finite values.
Results may differ from the reference program's by a relative error of at most 0.0003.
Values sent between devices are 32-bit elements; how exact they have to be, the bound alone decides.
A program may use at most 128 MiB of HBM per device.

```python
import math
from functools import partial
import jax
import jax.numpy as jnp
from jax import lax

NODES = 4096
SCENARIOS = 96
POLES = 6
STEPS = 3
DELAY_MAX = 4
SLOTS = 512
SUBS = 4
LINE_SLOTS = 4096
N_LINE = 8


def pair_tables(key):
    devices = SUBS * (LINE_SLOTS // SLOTS)
    anchor = jax.random.randint(jax.random.fold_in(key, 101), (), 0, devices)
    others = jax.random.permutation(jax.random.fold_in(key, 102), devices - 2) + 2
    flip_table = jnp.concatenate([jnp.ones((1,), jnp.int32), others.astype(jnp.int32)])
    slot_range = jnp.arange(SLOTS, dtype=jnp.int32)
    flip_mask = flip_table[slot_range % (devices - 1)]
    device_range = jnp.arange(devices, dtype=jnp.int32)
    partners = jnp.bitwise_xor(device_range[:, None], flip_mask[None, :])
    relabel = jnp.bitwise_xor(device_range, anchor)
    lowest = SLOTS // 6
    counts = jnp.where(relabel < 2, SLOTS, lowest + (relabel - 2) * (SLOTS - lowest) // (devices - 2))
    is_live = (slot_range[None, :] < counts[:, None]) & (slot_range[None, :] < counts[partners])
    return (partners, is_live, device_range, slot_range)


def draw_ownership(key, part):
    partners, is_live, device_range, slot_range = pair_tables(key)
    return is_live.astype(jnp.int32).reshape(SUBS, LINE_SLOTS)


def draw_partner(key, part):
    partners, is_live, device_range, slot_range = pair_tables(key)
    return partners.astype(jnp.int32).reshape(SUBS, LINE_SLOTS)


def draw_delay_steps(key, part):
    partners, is_live, device_range, slot_range = pair_tables(key)
    table = jax.random.randint(jax.random.fold_in(key, 103), partners.shape, 1, DELAY_MAX + 1)
    lower = jnp.minimum(device_range[:, None], partners)
    delays = table[lower, slot_range[None, :]]
    return delays.astype(jnp.int32).reshape(SUBS, LINE_SLOTS)


def draw_conductance_inverse(key, part):

    def one_block(index):
        block_key = jax.random.fold_in(key, index + 7)
        raw = jax.random.normal(jax.random.fold_in(block_key, 1), (NODES, NODES), jnp.float32)
        spread = (raw + raw.T) * (0.008 / math.sqrt(2.0))
        diagonal = jnp.exp(jax.random.uniform(jax.random.fold_in(block_key, 2), (NODES,), jnp.float32, math.log(1.5), math.log(4.0)))
        return spread + jnp.diag(diagonal)
    return lax.map(one_block, jnp.arange(SUBS, dtype=jnp.int32)).astype(jnp.float32)


def touch_ends(result, rng, smallest, high):
    longest = result.shape.index(max(result.shape))
    spots = []
    for shift in (0, 1):
        where = [jax.random.randint(jax.random.fold_in(rng, axis), (), 0, length) for axis, length in enumerate(result.shape)]
        where[longest] = (where[longest] + shift) % result.shape[longest]
        spots.append(tuple(where))
    return result.at[spots[0]].set(smallest).at[spots[1]].set(high)


def levels(own_key, extent, pieces, smallest, high):
    def one(axis_at, parts):
        draws = jax.random.uniform(jax.random.fold_in(jax.random.fold_in(own_key, 6), axis_at), (parts,), jnp.float32, smallest / len(pieces), high / len(pieces))
        return jnp.repeat(jnp.exp(draws), extent[axis_at] // parts).reshape((-1,) + (1,) * (len(extent) - axis_at - 1))

    loudness = one(*pieces[0])
    for cut in pieces[1:]:
        loudness = loudness * one(*cut)
    return loudness


def noise(own_key, dims, scale, bound, cuts=(), kind=jnp.bfloat16):
    loudness = levels(own_key, dims, cuts, -0.22, 0.18) if cuts else 1.0
    result = jax.random.normal(own_key, dims, jnp.float32) * scale * loudness
    return jnp.minimum(jnp.maximum(result, -bound), bound).astype(kind)


def setup_inputs(seed: int = 0) -> dict:
    splits = jax.random.split(jax.random.key(seed), 18)
    conductance_inverse = draw_conductance_inverse(jax.random.fold_in(splits[17], 71), 0)
    prior_voltage = noise(splits[1], (SUBS, SCENARIOS, NODES), 1.0, 6.0, ((0, 4), (2, 8)), jnp.float32)
    sources = noise(splits[2], (STEPS, SUBS, NODES), 1.0, 6.0, ((1, 4), (2, 8)), jnp.float32)
    fault_node = touch_ends(jax.random.randint(splits[3], (SCENARIOS,), 0, SUBS * NODES), jax.random.fold_in(splits[3], 1), 0, (SUBS * NODES) - 1).astype(jnp.int32)
    fault_conductance = jnp.clip(jnp.exp(jax.random.uniform(splits[4], (SCENARIOS,), jnp.float32, math.log(0.5), math.log(4.0))), 0.5, 4.0)
    terminal_node = touch_ends(jax.random.randint(splits[5], (SUBS, 3, LINE_SLOTS), 0, NODES), jax.random.fold_in(splits[5], 1), 0, NODES - 1).astype(jnp.int32)
    ownership = draw_ownership(jax.random.fold_in(splits[17], 71), 0)
    partner = draw_partner(jax.random.fold_in(splits[17], 71), 0)
    delay_steps = draw_delay_steps(jax.random.fold_in(splits[17], 71), 0)
    surge_conductance = jnp.clip(jnp.exp(math.log(1.0) - 1.609438 * jax.random.uniform(splits[9], (SUBS, LINE_SLOTS), jnp.float32) ** levels(splits[9], (SUBS, LINE_SLOTS), ((0, 4), (1, 8)), -0.2, 0.2)), 0.2, 1.0)
    pole_wave = jnp.clip(jnp.exp(math.log(0.95) - 1.5581446 * jax.random.uniform(splits[10], (SUBS, POLES, LINE_SLOTS), jnp.float32) ** levels(splits[10], (SUBS, POLES, LINE_SLOTS), ((0, 4), (2, 8)), -0.2, 0.2)), 0.2, 0.95)
    residue_wave = noise(splits[11], (SUBS, POLES, 3, 3, LINE_SLOTS), 0.15, 1.0, ((0, 4), (4, 8)), jnp.float32)
    pole_admit = jnp.clip(jnp.exp(math.log(0.95) - 1.5581446 * jax.random.uniform(splits[12], (SUBS, POLES, LINE_SLOTS), jnp.float32) ** levels(splits[12], (SUBS, POLES, LINE_SLOTS), ((0, 4), (2, 8)), -0.2, 0.2)), 0.2, 0.95)
    residue_admit = noise(splits[13], (SUBS, POLES, 3, 3, LINE_SLOTS), 0.15, 1.0, ((0, 4), (4, 8)), jnp.float32)
    wave_state = noise(splits[14], (SUBS, POLES, 3, SCENARIOS, LINE_SLOTS), 0.5, 4.0, ((0, 4), (4, 8)), jnp.float32)
    admit_state = noise(splits[15], (SUBS, POLES, 3, SCENARIOS, LINE_SLOTS), 0.5, 4.0, ((0, 4), (4, 8)), jnp.float32)
    wave_history = noise(splits[16], (SUBS, DELAY_MAX, 3, SCENARIOS, LINE_SLOTS), 1.0, 6.0, ((0, 4), (4, 8)), jnp.float32)
    return {"conductance_inverse": conductance_inverse, "prior_voltage": prior_voltage, "sources": sources, "fault_node": fault_node, "fault_conductance": fault_conductance, "terminal_node": terminal_node, "ownership": ownership, "partner": partner, "delay_steps": delay_steps, "surge_conductance": surge_conductance, "pole_wave": pole_wave, "residue_wave": residue_wave, "pole_admit": pole_admit, "residue_admit": residue_admit, "wave_state": wave_state, "admit_state": admit_state, "wave_history": wave_history}


def mix_residue(residue, vector):
    return (residue[:, :, 0, None, :] * vector[0] + residue[:, :, 1, None, :] * vector[1]
            + residue[:, :, 2, None, :] * vector[2])


def select_delayed(buffer, delay_local):
    depth_count = buffer.shape[0]
    chosen = delay_local[None, :] == jnp.arange(1, depth_count + 1, dtype=jnp.int32)[:, None]
    return jnp.sum(jnp.where(chosen[:, None, None, :], buffer, 0.0), axis=0)


def terminal_values(voltage, terminal):
    picked = jnp.take(voltage, terminal.reshape(-1), axis=1)
    return jnp.moveaxis(picked.reshape(voltage.shape[0], 3, -1), 0, 1)


def spread_ends(history, terminal, node_count):
    values = jnp.moveaxis(history, 0, 1).reshape(history.shape[1], -1)
    return jnp.zeros((history.shape[1], node_count), jnp.float32).at[:, terminal.reshape(-1)].add(values)


def split_devices(array):
    leading = array.shape[0]
    middle = array.shape[1:-1]
    shaped = array.reshape((leading,) + middle + (N_LINE, array.shape[-1] // N_LINE))
    shaped = jnp.moveaxis(shaped, -2, 1)
    return shaped.reshape((leading * N_LINE,) + middle + (shaped.shape[-1],))


def join_devices(array):
    leading = array.shape[0] // N_LINE
    middle = array.shape[1:-1]
    shaped = array.reshape((leading, N_LINE) + middle + (array.shape[-1],))
    shaped = jnp.moveaxis(shaped, 1, -2)
    return shaped.reshape((leading,) + middle + (N_LINE * array.shape[-1],))


def solve_block(operands):
    return lax.dot_general(operands[0], operands[1], (((1,), (1,)), ((), ())),
                           precision=lax.Precision.HIGHEST, preferred_element_type=jnp.float32)


def reference(conductance_inverse, prior_voltage, sources, fault_node, fault_conductance, terminal_node,
              ownership, partner, delay_steps, surge_conductance, pole_wave, residue_wave, pole_admit,
              residue_admit, wave_state, admit_state, wave_history):
    live_float = split_devices(ownership).astype(jnp.float32)
    terminal_dev = split_devices(terminal_node)
    partner_dev = split_devices(partner)
    delay_dev = split_devices(delay_steps)
    surge_dev = split_devices(surge_conductance)
    wave_decay = split_devices(pole_wave)[:, :, None, None, :]
    admit_decay = split_devices(pole_admit)[:, :, None, None, :]
    wave_res = split_devices(residue_wave)
    admit_res = split_devices(residue_admit)
    wave_now = split_devices(wave_state)
    admits = split_devices(admit_state)
    history_buffer = split_devices(wave_history)
    slot_count = live_float.shape[1]
    slot_range = jnp.arange(slot_count, dtype=jnp.int32)
    scenario_range = jnp.arange(prior_voltage.shape[1], dtype=jnp.int32)
    fault_sub = fault_node // NODES
    fault_local = fault_node % NODES
    voltage = prior_voltage
    outgoing = None
    current = None
    mixer = jax.vmap(mix_residue)
    for step_index in range(STEPS):
        if step_index > 0:
            by_slot = jnp.moveaxis(outgoing, 3, 1)
            far_waves = by_slot[partner_dev, slot_range[None, :]]
            arrived = jnp.moveaxis(far_waves, 1, 3) * live_float[:, None, None, :]
            history_buffer = jnp.concatenate([arrived[:, None], history_buffer[:, :-1]], axis=1)
        incoming = jax.vmap(select_delayed)(history_buffer, delay_dev)
        voltage_dev = jnp.repeat(voltage, N_LINE, axis=0)
        terminal_prior = jax.vmap(terminal_values)(voltage_dev, terminal_dev)
        wave_now = wave_decay * wave_now + mixer(wave_res, incoming)
        admits = admit_decay * admits + mixer(admit_res, terminal_prior)
        history = (jnp.sum(wave_now, axis=1) - jnp.sum(admits, axis=1)) * live_float[:, None, None, :]
        injection = jax.vmap(partial(spread_ends, node_count=NODES))(join_devices(history), terminal_node)
        injection = injection + sources[step_index][:, None, :]
        fault_value = voltage[fault_sub, scenario_range, fault_local]
        injection = injection.at[fault_sub, scenario_range, fault_local].add(-fault_conductance * fault_value)
        voltage = lax.map(solve_block, (injection, conductance_inverse))
        voltage_dev = jnp.repeat(voltage, N_LINE, axis=0)
        terminal_now = jax.vmap(terminal_values)(voltage_dev, terminal_dev)
        if step_index + 1 < STEPS:
            outgoing = (2.0 * surge_dev[:, None, None, :] * terminal_now - history) * live_float[:, None, None, :]
        else:
            current = (surge_dev[:, None, None, :] * terminal_now - history) * live_float[:, None, None, :]
    return voltage, join_devices(current)
```

```python
import functools

import jax
import jax.numpy as jnp
from jax import lax
from jax.experimental import pallas as pl
from jax.experimental.pallas import tpu as pltpu
from jax.sharding import PartitionSpec as P

STEPS = 3
CORES = 2
SPLIT = 2
LANES = 128
SUBLANES = 8
MESH = pl.DeviceIdType.MESH


def split_two(value):
    high = value.astype(jnp.bfloat16)
    low = (value - high.astype(jnp.float32)).astype(jnp.bfloat16)
    return high, low


def stack_two(value):
    return jnp.concatenate(split_two(value), axis=0)


def fold_two(value):
    half = value.shape[0] // 2
    return value[:half] + value[half:]


def dot_nt(left, right):
    return lax.dot_general(left, right, (((1,), (1,)), ((), ())), preferred_element_type=jnp.float32)


def dot_nn(left, right):
    return lax.dot_general(left, right, (((1,), (0,)), ((), ())), preferred_element_type=jnp.float32)


def as_hot(mask):
    return mask.astype(jnp.float32).astype(jnp.bfloat16)


def message_plan(capacity, width):
    tiles, rest = width // LANES, width % LANES
    groups = LANES // rest
    base = capacity // SUBLANES * SUBLANES
    spare = (capacity - base) * tiles
    left = -(-(spare + -(-capacity // groups)) // SUBLANES) * SUBLANES
    return tiles, rest, groups, base, spare, left


def kernel(
    lines, nets,
    prior_ref, source_ref, fnode_ref, fcond_ref, term_ref, live_ref, partner_ref, delay_ref, surge_ref,
    polew_ref, resw_ref, polea_ref, resa_ref, inv_hbm, wave_hbm, admit_hbm, hist_hbm,
    volt_ref, curr_ref,
    inv, wave, admit, hist, inv_high, inv_low, hot, pack_main, pack_left, left_rhs,
    coef_w, coef_a, hist_sum, ends, h, h_split, fault, ifull, vfull,
    part, r1, mine, rbuf, xsend, xrecv,
    load_sem, a_send, a_recv, b_send, b_recv,
    ic_send, ic_recv, id_send, id_recv, vc_send, vc_recv, vd_send, vd_recv, x_send, x_recv,
):
    chips = lines // CORES
    devices = lines * nets
    net = lax.axis_index("net")
    line = lax.axis_index("line")
    z = line // CORES
    core = lax.rem(line, CORES)
    me = net * lines + line
    mate = z * CORES + 1 - core
    phases, count, slots = h.shape
    width = ifull.shape[2]
    nodes = width * lines
    half = count // SPLIT
    capacity = (slots + devices - 2) // (devices - 1)
    tiles, rest, groups, base, spare, left = message_plan(capacity, phases * count)
    lead = tiles * base

    def remote(src, dst, send, recv, target):
        return pltpu.make_async_remote_copy(
            src_ref=src, dst_ref=dst, send_sem=send, recv_sem=recv,
            device_id={"line": target}, device_id_type=MESH,
        )

    def nearest(e):
        near = jnp.minimum(z, chips - 1 - z)
        both = jnp.where(lax.rem(e, 2) == 1, z - (e + 1) // 2, z + e // 2)
        one = jnp.where(z > near, z - (e - near), z + (e - near))
        return jnp.where(e <= 2 * near, both, one)

    def rows(s):
        return pl.ds(s * half, half)

    loads = [
        pltpu.make_async_copy(src, dst, load_sem.at[i])
        for i, (src, dst) in enumerate(
            ((wave_hbm, wave), (admit_hbm, admit), (hist_hbm, hist), (inv_hbm, inv))
        )
    ]
    for load in loads:
        load.start()

    barrier = pltpu.get_barrier_semaphore()

    def greet(i, carry):
        peer = lax.rem(me + 1 + i, devices)
        pl.semaphore_signal(
            barrier, inc=1, device_id={"net": peer // lines, "line": lax.rem(peer, lines)},
            device_id_type=MESH,
        )
        return carry

    lax.fori_loop(0, devices - 1, greet, 0)
    vfull[line] = prior_ref[...]
    ends[...] = jnp.zeros_like(ends)
    xrecv[:, me] = jnp.zeros_like(xrecv[:, me])
    left_rhs[...] = jnp.zeros_like(left_rhs)
    pl.semaphore_wait(barrier, devices - 1)

    def gather_start(buf, sems):
        c_send, c_recv, d_send, d_recv = sems
        for s in range(SPLIT):
            view = buf.at[line, rows(s)]

            @pl.when(z + 1 < chips)
            def _():
                remote(view, view, c_send.at[0, z, s], c_recv.at[z, s], line + CORES).start()

            @pl.when(z > 0)
            def _():
                remote(view, view, c_send.at[1, z, s], c_recv.at[z, s], line - CORES).start()

            remote(view, view, d_send.at[z, s], d_recv.at[z, s], mate).start()

    def gather(buf, sems, consume, fill=None):
        c_send, c_recv, d_send, d_recv = sems

        def step(e, carry):
            source = nearest(e)
            block = source * CORES + core
            other = source * CORES + 1 - core

            @pl.when(e > 0)
            def _():
                for s in range(SPLIT):
                    view = buf.at[block, rows(s)]
                    remote(view, view, c_send.at[0, source, s], c_recv.at[source, s], mate).wait_recv()

                    @pl.when((source < z) & (z + 1 < chips))
                    def _():
                        remote(view, view, c_send.at[0, source, s], c_recv.at[source, s], line + CORES).start()

                    @pl.when((source > z) & (z > 0))
                    def _():
                        remote(view, view, c_send.at[1, source, s], c_recv.at[source, s], line - CORES).start()

                    remote(view, view, d_send.at[source, s], d_recv.at[source, s], mate).start()

            if fill is not None:
                fill(e)

            def take(j, carry):
                @pl.when(j == 1)
                def _():
                    for s in range(SPLIT):
                        view = buf.at[other, rows(s)]
                        remote(view, view, d_send.at[source, s], d_recv.at[source, s], mate).wait_recv()

                consume(source * CORES + lax.rem(core + j, CORES))
                return carry

            lax.fori_loop(0, CORES, take, 0)
            return carry

        lax.fori_loop(0, chips, step, 0)

        def drain(source, carry):
            block = source * CORES + core
            for s in range(SPLIT):
                view = buf.at[block, rows(s)]
                remote(view, view, d_send.at[source, s], d_recv.at[source, s], mate).wait_send()

                @pl.when((source <= z) & (z + 1 < chips))
                def _():
                    remote(view, view, c_send.at[0, source, s], c_recv.at[source, s], mate).wait_send()

                @pl.when((source >= z) & (z > 0))
                def _():
                    remote(view, view, c_send.at[1, source, s], c_recv.at[source, s], mate).wait_send()

            return carry

        lax.fori_loop(0, chips, drain, 0)

    def pick(block):
        both = stack_two(vfull[block])
        for p in range(phases):
            ends[p] += fold_two(dot_nn(both, hot[p, block]))

    def spread(block):
        total = jnp.zeros((count, width), jnp.float32)
        for p in range(phases):
            total = total + fold_two(dot_nt(h_split[p], hot[p, block]))
        return total

    def solve(block):
        both = stack_two(ifull[block])
        got = dot_nt(both, inv_high[block])
        volt_ref[...] += got[:count] + (got[count:] + dot_nt(both[:count], inv_low[block]))

    def build_hot():
        def one(block, carry):
            lane = lax.broadcasted_iota(jnp.int32, (width, slots), 0) + block * width
            for p in range(phases):
                hot[p, block] = as_hot(lane == term_ref[p : p + 1, :])
            return carry

        lax.fori_loop(0, lines, one, 0)

    def build_inverse():
        loads[3].wait()

        def one(block, carry):
            high, low = split_two(inv[:, pl.ds(pl.multiple_of(block * width, width), width)])
            inv_high[block] = high
            inv_low[block] = low
            return carry

        lax.fori_loop(0, lines, one, 0)

    def build_coef():
        poles = polew_ref.shape[0]
        for pole_ref, res_ref, coef in ((polew_ref, resw_ref, coef_w), (polea_ref, resa_ref, coef_a)):
            for p in range(phases):
                for r in range(phases):
                    power = [res_ref[q, p, r : r + 1, :] for q in range(poles)]
                    for m in range(STEPS):
                        total = power[0]
                        for q in range(1, poles):
                            total = total + power[q]
                        coef[m, p * phases + r : p * phases + r + 1, :] = total
                        if m + 1 < STEPS:
                            power = [power[q] * pole_ref[q : q + 1, :] for q in range(poles)]

    def build_history():
        for load in loads[:3]:
            load.wait()
        poles = polew_ref.shape[0]
        depth = hist.shape[0]
        delay = delay_ref[...]
        groups_of_rows = count // SUBLANES

        def one(g, carry):
            at = pl.ds(pl.multiple_of(g * SUBLANES, SUBLANES), SUBLANES)
            old = []
            for t in range(1, STEPS + 1):
                per_phase = []
                for r in range(phases):
                    value = jnp.zeros((SUBLANES, slots), jnp.float32)
                    for d in range(t, depth + 1):
                        value = jnp.where(delay == d, hist[d - t, r, at, :], value)
                    per_phase.append(value)
                old.append(per_phase)
            for p in range(phases):
                sums = [jnp.zeros((SUBLANES, slots), jnp.float32) for _ in range(STEPS)]
                for q in range(poles):
                    x = wave[q, p, at, :]
                    y = admit[q, p, at, :]
                    for t in range(STEPS):
                        x = x * polew_ref[q : q + 1, :]
                        y = y * polea_ref[q : q + 1, :]
                        sums[t] = sums[t] + (x - y)
                for t in range(STEPS):
                    for s in range(t + 1):
                        for r in range(phases):
                            row = p * phases + r
                            sums[t] = sums[t] + coef_w[t - s, row : row + 1, :] * old[s][r]
                    hist_sum[t, p, at, :] = sums[t]
            return carry

        lax.fori_loop(0, groups_of_rows, one, 0)

    def build_packers():
        owner = lax.broadcasted_iota(jnp.int32, (devices, slots), 0)
        hits = as_hot((owner == partner_ref[...]) & (live_ref[...] > 0))
        before = as_hot(
            lax.broadcasted_iota(jnp.int32, (slots, slots), 0)
            < lax.broadcasted_iota(jnp.int32, (slots, slots), 1)
        )
        counts = dot_nn(hits, before) * hits.astype(jnp.float32)
        rank = jnp.sum(counts, axis=0, keepdims=True).astype(jnp.int32)
        stride = slots
        place = jnp.where(live_ref[...] > 0, partner_ref[...] * stride + rank, -1)
        if base:
            row = lax.broadcasted_iota(jnp.int32, (devices * base, slots), 0)
            pack_main[...] = as_hot((row // base) * stride + lax.rem(row, base) == place)
        row = lax.broadcasted_iota(jnp.int32, (devices * left, slots), 0)
        owner = row // left
        index = lax.rem(row, left)
        for k in range(groups + tiles):
            if k < groups:
                wanted = (index - spare) * groups + k
                fits = (index >= spare) & (wanted < capacity)
            else:
                wanted = base + index // tiles
                fits = (index < spare) & (lax.rem(index, tiles) == k - groups)
            wanted = jnp.where(fits, owner * stride + wanted, -2)
            pack_left[:, k * slots : (k + 1) * slots] = as_hot(wanted == place)

    def build_fault():
        local = fnode_ref[...] - (net * nodes + line * width)
        lane = lax.broadcasted_iota(jnp.int32, (count, width), 1)
        fault[...] = jnp.where(lane == local, fcond_ref[...], 0.0)

    def fill_prior(e):
        @pl.when(e == 0)
        def _():
            build_hot()

        @pl.when(e == 1)
        def _():
            build_coef()
            build_fault()

        @pl.when(e == 2)
        def _():
            build_inverse()

        @pl.when(e == chips - 1)
        def _():
            build_history()
            build_packers()

    def scatter_sum():
        def finish(e):
            target = nearest(chips - 1 - e)
            remote(part.at[target], r1.at[target], a_send.at[target], a_recv.at[target], mate).wait_recv()
            mine[target] = mine[target] + r1[target]
            pass_on(target, (z == 0) & (target > z), (z == chips - 1) & (target < z))

        def pass_on(target, right, left_way):
            for s in range(SPLIT):
                pass_half(target, s, right, left_way)

        def pass_half(target, s, right, left_way):
            @pl.when(right)
            def _():
                remote(
                    mine.at[target, rows(s)], rbuf.at[0, target, rows(s)],
                    b_send.at[target, s], b_recv.at[0, target, s], line + CORES,
                ).start()

            @pl.when(left_way)
            def _():
                remote(
                    mine.at[target, rows(s)], rbuf.at[1, target, rows(s)],
                    b_send.at[target, s], b_recv.at[1, target, s], line - CORES,
                ).start()

        def compute(e, carry):
            target = nearest(chips - 1 - e)

            def both(j, carry):
                got = spread(target * CORES + lax.rem(core + 1 + j, CORES))

                @pl.when(j == 0)
                def _():
                    part[target] = got
                    remote(
                        part.at[target], r1.at[target], a_send.at[target], a_recv.at[target], mate
                    ).start()

                @pl.when(j == 1)
                def _():
                    mine[target] = got

                return carry

            lax.fori_loop(0, CORES, both, 0)

            @pl.when(e > 0)
            def _():
                finish(e - 1)

            return carry

        lax.fori_loop(0, chips, compute, 0)
        finish(chips - 1)

        def arrive(side, target, s):
            remote(
                mine.at[target, rows(s)], rbuf.at[side, target, rows(s)],
                b_send.at[target, s], b_recv.at[side, target, s], mate,
            ).wait_recv()
            mine[target, rows(s)] = mine[target, rows(s)] + rbuf[side, target, rows(s)]

        def relay(e, carry):
            target = nearest(chips - 1 - e)
            for s in range(SPLIT):
                @pl.when((target >= z) & (z > 0))
                def _():
                    arrive(0, target, s)

                @pl.when((target <= z) & (z + 1 < chips))
                def _():
                    arrive(1, target, s)

                pass_half(target, s, (target > z) & (z > 0), (target < z) & (z + 1 < chips))
            return carry

        lax.fori_loop(0, chips, relay, 0)

    def scatter_drain():
        def one(target, carry):
            remote(part.at[target], r1.at[target], a_send.at[target], a_recv.at[target], mate).wait_send()

            @pl.when(target < z)
            def _():
                for s in range(SPLIT):
                    remote(
                        mine.at[target, rows(s)], rbuf.at[0, target, rows(s)],
                        b_send.at[target, s], b_recv.at[0, target, s], mate,
                    ).wait_send()

            @pl.when(target > z)
            def _():
                for s in range(SPLIT):
                    remote(
                        mine.at[target, rows(s)], rbuf.at[0, target, rows(s)],
                        b_send.at[target, s], b_recv.at[0, target, s], mate,
                    ).wait_send()

            return carry

        lax.fori_loop(0, chips, one, 0)

    def exchange_copy(t, i):
        peer = lax.rem(me + 1 + i, devices)
        return pltpu.make_async_remote_copy(
            src_ref=xsend.at[peer], dst_ref=xrecv.at[t, me], send_sem=x_send.at[i],
            recv_sem=x_recv.at[t, i],
            device_id={"net": peer // lines, "line": lax.rem(peer, lines)}, device_id_type=MESH,
        )

    def exchange_start(t):
        surge = surge_ref[...]
        live = live_ref[...].astype(jnp.float32)
        wave_out = jnp.concatenate(
            [(2.0 * surge * ends[p] - h[p]) * live for p in range(phases)], axis=0
        )
        high, low = split_two(wave_out)
        body = tiles * LANES
        if base:
            main = dot_nt(pack_main[...], jnp.concatenate([high[:body], low[:body]], axis=0))
            main = main[:, :body] + main[:, body:]
            for j in range(tiles):
                xsend[:, j * base : (j + 1) * base, :] = main[:, j * LANES : (j + 1) * LANES].reshape(
                    devices, base, LANES
                )
        for offset, value in ((0, high), (LANES, low)):
            for k in range(groups):
                left_rhs[offset + k * rest : offset + (k + 1) * rest, k * slots : (k + 1) * slots] = value[body:]
            for j in range(tiles):
                left_rhs[offset : offset + LANES, (groups + j) * slots : (groups + j + 1) * slots] = value[
                    j * LANES : (j + 1) * LANES
                ]
        tail = dot_nt(pack_left[...], left_rhs[...])
        tail = tail[:, :LANES] + tail[:, LANES:]
        xsend[:, lead : lead + left, :] = tail.reshape(devices, left, LANES)

        def go(i, carry):
            exchange_copy(t, i).start()
            return carry

        lax.fori_loop(0, devices - 1, go, 0)

    def exchange_finish(t):
        def end(i, carry):
            exchange_copy(t, i).wait()
            return carry

        lax.fori_loop(0, devices - 1, end, 0)

    def unpack(t):
        tail = xrecv[t, :, lead : lead + left, :].reshape(devices * left, LANES).T
        high, low = split_two(tail)
        arrived = []
        if base:
            for j in range(tiles):
                main = xrecv[t, :, j * base : (j + 1) * base, :].reshape(devices * base, LANES).T
                arrived.append(fold_two(dot_nn(stack_two(main), pack_main[...])))
        for j in range(tiles):
            k = groups + j
            more = fold_two(
                dot_nn(jnp.concatenate([high, low], axis=0), pack_left[:, k * slots : (k + 1) * slots])
            )
            if base:
                arrived[j] = arrived[j] + more
            else:
                arrived.append(more)
        last = jnp.zeros((rest, slots), jnp.float32)
        for k in range(groups):
            here = slice(k * rest, (k + 1) * rest)
            last = last + fold_two(
                dot_nn(jnp.concatenate([high[here], low[here]], axis=0), pack_left[:, k * slots : (k + 1) * slots])
            )
        return jnp.concatenate(arrived + [last], axis=0)

    def mixed(coef, m, p, values):
        total = coef[m, p * phases : p * phases + 1, :] * values[0]
        for r in range(1, phases):
            total = total + coef[m, p * phases + r : p * phases + r + 1, :] * values[r]
        return total

    def add_ends(t):
        values = [ends[r] for r in range(phases)]
        for m in range(STEPS):
            @pl.when(t + m < STEPS)
            def _():
                for p in range(phases):
                    hist_sum[t + m, p] = hist_sum[t + m, p] - mixed(coef_a, m, p, values)

    def add_waves(t):
        arrived = unpack(t - 1)
        delay = delay_ref[...]
        for d in range(1, STEPS):
            values = [
                jnp.where(delay == d, arrived[r * count : (r + 1) * count], 0.0) for r in range(phases)
            ]
            for m in range(STEPS - d):
                @pl.when(t + d - 1 + m < STEPS)
                def _():
                    for p in range(phases):
                        at = t + d - 1 + m
                        hist_sum[at, p] = hist_sum[at, p] + mixed(coef_w, m, p, values)

    isems = (ic_send, ic_recv, id_send, id_recv)
    vsems = (vc_send, vc_recv, vd_send, vd_recv)
    gather_start(vfull, vsems)
    gather(vfull, vsems, pick, fill_prior)

    def run_step(t, carry):
        add_ends(t)

        @pl.when(t > 0)
        def _():
            exchange_finish(t - 1)
            add_waves(t)

        live = live_ref[...].astype(jnp.float32)
        for p in range(phases):
            now = hist_sum[t, p] * live
            h[p] = now
            h_split[p] = stack_two(now)
        extra = source_ref[t] - fault[...] * vfull[line]
        scatter_sum()
        ifull[line] = mine[z] + extra
        gather_start(ifull, isems)
        volt_ref[...] = jnp.zeros_like(volt_ref)
        gather(ifull, isems, solve)
        vfull[line] = volt_ref[...]
        gather_start(vfull, vsems)
        scatter_drain()
        ends[...] = jnp.zeros_like(ends)
        gather(vfull, vsems, pick)

        @pl.when(t + 1 < STEPS)
        def _():
            exchange_start(t)

        return carry

    lax.fori_loop(0, STEPS, run_step, 0)
    live = live_ref[...].astype(jnp.float32)
    for p in range(phases):
        curr_ref[p] = (surge_ref[...] * ends[p] - h[p]) * live


def on_device(
    conductance_inverse, prior_voltage, sources, fault_node, fault_conductance, terminal_node,
    ownership, partner, delay_steps, surge_conductance, pole_wave, residue_wave, pole_admit,
    residue_admit, wave_state, admit_state, wave_history,
):
    lines = lax.axis_size("line")
    nets = lax.axis_size("net")
    devices = lines * nets
    chips = lines // CORES
    inverse = conductance_inverse[0]
    prior = prior_voltage[0]
    terminal = terminal_node[0]
    count, width = prior.shape
    phases, slots = terminal.shape
    wave = wave_state[0]
    admit = admit_state[0]
    hist = wave_history[0]
    capacity = (slots + devices - 2) // (devices - 1)
    tiles, rest, groups, base, spare, left = message_plan(capacity, phases * count)
    message = tiles * base + left
    f32, bf16 = jnp.float32, jnp.bfloat16
    vmem = lambda: pl.BlockSpec(memory_space=pltpu.VMEM)
    hbm = lambda: pl.BlockSpec(memory_space=pltpu.HBM)
    dma = lambda *shape: pltpu.SemaphoreType.DMA(shape)
    gather_sems = [
        dma(2, chips, SPLIT), dma(chips, SPLIT), dma(chips, SPLIT), dma(chips, SPLIT),
    ]
    volt, curr = pl.pallas_call(
        functools.partial(kernel, lines, nets),
        out_shape=(
            jax.ShapeDtypeStruct((count, width), f32),
            jax.ShapeDtypeStruct((phases, count, slots), f32),
        ),
        in_specs=[vmem()] * 13 + [hbm()] * 4,
        out_specs=(vmem(), vmem()),
        scratch_shapes=[
            pltpu.VMEM(inverse.shape, f32),
            pltpu.VMEM(wave.shape, f32),
            pltpu.VMEM(admit.shape, f32),
            pltpu.VMEM(hist.shape, f32),
            pltpu.VMEM((lines, inverse.shape[0], width), bf16),
            pltpu.VMEM((lines, inverse.shape[0], width), bf16),
            pltpu.VMEM((phases, lines, width, slots), bf16),
            pltpu.VMEM((devices * max(base, SUBLANES), slots), bf16),
            pltpu.VMEM((devices * left, (groups + tiles) * slots), bf16),
            pltpu.VMEM((2 * LANES, (groups + tiles) * slots), bf16),
            pltpu.VMEM((STEPS, phases * phases, slots), f32),
            pltpu.VMEM((STEPS, phases * phases, slots), f32),
            pltpu.VMEM((STEPS, phases, count, slots), f32),
            pltpu.VMEM((phases, count, slots), f32),
            pltpu.VMEM((phases, count, slots), f32),
            pltpu.VMEM((phases, 2 * count, slots), bf16),
            pltpu.VMEM((count, width), f32),
            pltpu.VMEM((lines, count, width), f32),
            pltpu.VMEM((lines, count, width), f32),
            pltpu.VMEM((chips, count, width), f32),
            pltpu.VMEM((chips, count, width), f32),
            pltpu.VMEM((chips, count, width), f32),
            pltpu.VMEM((2, chips, count, width), f32),
            pltpu.VMEM((devices, message, LANES), f32),
            pltpu.VMEM((STEPS - 1, devices, message, LANES), f32),
            dma(4), dma(chips), dma(chips), dma(chips, SPLIT), dma(2, chips, SPLIT),
        ] + gather_sems + gather_sems + [dma(devices), dma(STEPS - 1, devices)],
        compiler_params=pltpu.CompilerParams(
            collective_id=0, has_side_effects=True, vmem_limit_bytes=67043328
        ),
        name="network",
    )(
        prior, sources, fault_node[:, None], fault_conductance[:, None], terminal, ownership, partner,
        delay_steps, surge_conductance, pole_wave[0], residue_wave[0], pole_admit[0], residue_admit[0],
        inverse, wave, admit, hist,
    )
    return volt[None], curr[None]


def solution(mesh):
    return jax.shard_map(
        on_device,
        mesh=mesh,
        in_specs=(
            P("net", "line", None),
            P("net", None, "line"),
            P(None, "net", "line"),
            P(),
            P(),
            P("net", None, "line"),
            P("net", "line"),
            P("net", "line"),
            P("net", "line"),
            P("net", "line"),
            P("net", None, "line"),
            P("net", None, None, None, "line"),
            P("net", None, "line"),
            P("net", None, None, None, "line"),
            P("net", None, None, None, "line"),
            P("net", None, None, None, "line"),
            P("net", None, None, None, "line"),
        ),
        out_specs=(P("net", None, "line"), P("net", None, None, "line")),
        check_vma=False,
    )
```

```python
import functools

import jax
import jax.numpy as jnp
from jax import lax
from jax.experimental import pallas as pl
from jax.experimental.pallas import tpu as pltpu
from jax.sharding import PartitionSpec as P

STEPS = 3
CORES = 2
SPLIT = 2
PIECES = 3
LANES = 128
SUBLANES = 8
MESH = pl.DeviceIdType.MESH


def split_two(value):
    high = value.astype(jnp.bfloat16)
    low = (value - high.astype(jnp.float32)).astype(jnp.bfloat16)
    return high, low


def stack_two(value):
    return jnp.concatenate(split_two(value), axis=0)


def fold_two(value):
    half = value.shape[0] // 2
    return value[:half] + value[half:]


def dot_nt(left, right):
    return lax.dot_general(left, right, (((1,), (1,)), ((), ())), preferred_element_type=jnp.float32)


def dot_nn(left, right):
    return lax.dot_general(left, right, (((1,), (0,)), ((), ())), preferred_element_type=jnp.float32)


def as_hot(mask):
    return mask.astype(jnp.float32).astype(jnp.bfloat16)


def message_plan(capacity, width):
    tiles, rest = width // LANES, width % LANES
    groups = LANES // rest
    base = capacity // SUBLANES * SUBLANES
    spare = (capacity - base) * tiles
    left = -(-(spare + -(-capacity // groups)) // SUBLANES) * SUBLANES
    return tiles, rest, groups, base, spare, left


def kernel(
    lines, nets,
    prior_ref, source_ref, fnode_ref, fcond_ref, term_ref, live_ref, partner_ref, delay_ref, surge_ref,
    polew_ref, resw_ref, polea_ref, resa_ref, inv_hbm, wave_hbm, admit_hbm, hist_hbm,
    volt_ref, curr_ref,
    wave, admit, hist, inv_high, inv_low, hot, hot_t, pack_main, pack_left, left_rhs,
    coef_w, coef_a, hist_sum, ends, h, h_split, fault, ifull, vfull,
    part, r1, mine, rbuf, xsend, xrecv,
    load_sem, inv_sem, a_send, a_recv, b_send, b_recv,
    ic_send, ic_recv, id_send, id_recv, vc_send, vc_recv, vd_send, vd_recv, x_send, x_recv,
):
    chips = lines // CORES
    devices = lines * nets
    net = lax.axis_index("net")
    line = lax.axis_index("line")
    z = line // CORES
    core = lax.rem(line, CORES)
    me = net * lines + line
    mate = z * CORES + 1 - core
    phases, count, slots = h.shape
    width = ifull.shape[2]
    nodes = width * lines
    half = count // SPLIT
    piece = half // PIECES
    poles = polew_ref.shape[0]
    depth = hist.shape[0] // (phases * count)
    capacity = (slots + devices - 2) // (devices - 1)
    tiles, rest, groups, base, spare, left = message_plan(capacity, phases * half)
    lead = tiles * base
    turned = len(hot_t.shape) == 4

    def remote(src, dst, send, recv, target):
        return pltpu.make_async_remote_copy(
            src_ref=src, dst_ref=dst, send_sem=send, recv_sem=recv,
            device_id={"line": target}, device_id_type=MESH,
        )

    def nearest(e):
        near = jnp.minimum(z, chips - 1 - z)
        both = jnp.where(lax.rem(e, 2) == 1, z - (e + 1) // 2, z + e // 2)
        one = jnp.where(z > near, z - (e - near), z + (e - near))
        return jnp.where(e <= 2 * near, both, one)

    def rows(s):
        return pl.ds(pl.multiple_of(s * half, half), half)

    def bits(s, i):
        return pl.ds(pl.multiple_of(s * half + i * piece, piece), piece)

    states = ((wave_hbm, wave), (admit_hbm, admit), (hist_hbm, hist))
    loads = [pltpu.make_async_copy(src, dst, load_sem.at[i]) for i, (src, dst) in enumerate(states)]
    for load in loads:
        load.start()

    places = [(dst, at) for _, dst in states for at in range(0, dst.shape[0] - width + 1, width)][:lines]

    def stage(block):
        dst, at = places[block]
        return pltpu.make_async_copy(
            inv_hbm.at[:, pl.ds(block * width, width)], dst.at[pl.ds(at, width), pl.ds(0, width)],
            inv_sem.at[block],
        )

    barrier = pltpu.get_barrier_semaphore()

    def greet(i, carry):
        peer = lax.rem(me + 1 + i, devices)
        pl.semaphore_signal(
            barrier, inc=1, device_id={"net": peer // lines, "line": lax.rem(peer, lines)},
            device_id_type=MESH,
        )
        return carry

    lax.fori_loop(0, devices - 1, greet, 0)
    vfull[line] = prior_ref[...]
    xrecv[:, :, me] = jnp.zeros_like(xrecv[:, :, me])

    def gather_hop(buf, sems, block, source, s, i, side, to):
        view = buf.at[block, bits(s, i)]
        return remote(view, view, sems[0].at[side, source, s, i], sems[1].at[source, s, i], to)

    def gather_start(buf, sems, s):
        c_send, c_recv, d_send, d_recv = sems

        @pl.when(z + 1 < chips)
        def _():
            for i in range(PIECES):
                gather_hop(buf, sems, line, z, s, i, 0, line + CORES).start()

        @pl.when(z > 0)
        def _():
            for i in range(PIECES):
                gather_hop(buf, sems, line, z, s, i, 1, line - CORES).start()

        view = buf.at[line, rows(s)]
        remote(view, view, d_send.at[z, s], d_recv.at[z, s], mate).start()

    def gather_arrive(buf, sems, s, e):
        c_send, c_recv, d_send, d_recv = sems
        source = nearest(e)
        block = source * CORES + core

        @pl.when(e > 0)
        def _():
            for i in range(PIECES):
                gather_hop(buf, sems, block, source, s, i, 0, mate).wait_recv()

                @pl.when((source < z) & (z + 1 < chips))
                def _():
                    gather_hop(buf, sems, block, source, s, i, 0, line + CORES).start()

                @pl.when((source > z) & (z > 0))
                def _():
                    gather_hop(buf, sems, block, source, s, i, 1, line - CORES).start()

            view = buf.at[block, rows(s)]
            remote(view, view, d_send.at[source, s], d_recv.at[source, s], mate).start()

    def gather_take(buf, sems, s, e, consume):
        c_send, c_recv, d_send, d_recv = sems

        def take(j, carry):
            source = nearest(jnp.maximum(e - j, 0))

            @pl.when((e < chips) & (j == 0))
            def _():
                consume(source * CORES + core, s)

            @pl.when((e > 0) & (j == 1))
            def _():
                view = buf.at[source * CORES + 1 - core, rows(s)]
                remote(view, view, d_send.at[source, s], d_recv.at[source, s], mate).wait_recv()
                consume(source * CORES + 1 - core, s)

            return carry

        lax.fori_loop(0, CORES, take, 0)

    def gather_last(buf, sems, s, consume):
        source = nearest(chips - 1)
        view = buf.at[source * CORES + 1 - core, rows(s)]
        remote(view, view, sems[2].at[source, s], sems[3].at[source, s], mate).wait_recv()
        consume(source * CORES + 1 - core, s)

    def gather_drain(buf, sems, s):
        c_send, c_recv, d_send, d_recv = sems

        def drain(source, carry):
            block = source * CORES + core
            view = buf.at[block, rows(s)]
            remote(view, view, d_send.at[source, s], d_recv.at[source, s], mate).wait_send()

            @pl.when((source <= z) & (z + 1 < chips))
            def _():
                for i in range(PIECES):
                    gather_hop(buf, sems, block, source, s, i, 0, mate).wait_send()

            @pl.when((source >= z) & (z > 0))
            def _():
                for i in range(PIECES):
                    gather_hop(buf, sems, block, source, s, i, 1, mate).wait_send()

            return carry

        lax.fori_loop(0, chips, drain, 0)

    def pick(block, s):
        both = stack_two(vfull[block, rows(s)])
        for p in range(phases):
            ends[p, rows(s)] += fold_two(dot_nn(both, hot[p, block]))

    def spread(block, s):
        total = jnp.zeros((half, width), jnp.float32)
        for p in range(phases):
            if turned:
                total = total + fold_two(dot_nn(h_split[p], hot_t[p, block]))
            else:
                total = total + fold_two(dot_nt(h_split[p], hot[p, block]))
        return total

    def solve(block, s):
        both = stack_two(ifull[block, rows(s)])
        got = dot_nn(both, inv_high[block])
        volt_ref[rows(s)] += got[:half] + (got[half:] + dot_nn(both[:half], inv_low[block]))

    def build_hot():
        def one(block, carry):
            lane = lax.broadcasted_iota(jnp.int32, (width, slots), 0) + block * width
            for p in range(phases):
                hot[p, block] = as_hot(lane == term_ref[p])
            return carry

        lax.fori_loop(0, lines, one, 0)

    def build_hot_t():
        for p in range(phases):
            tall = jnp.broadcast_to(term_ref[p].astype(jnp.float32), (LANES, slots)).T.astype(jnp.int32)
            lane = lax.broadcasted_iota(jnp.int32, (slots, LANES), 1)

            def one(block, carry):
                for j in range(width // LANES):
                    hot_t[p, block, :, j * LANES : (j + 1) * LANES] = as_hot(
                        lane + (block * width + j * LANES) == tall
                    )
                return carry

            lax.fori_loop(0, lines, one, 0)

    def build_inverse():
        for block in range(lines):
            dst, at = places[block]
            stage(block).wait()
            high, low = split_two(dst[pl.ds(at, width), :width].T)
            inv_high[block] = high
            inv_low[block] = low

    def build_coef():
        for pole_ref, res_ref, coef in ((polew_ref, resw_ref, coef_w), (polea_ref, resa_ref, coef_a)):
            for p in range(phases):
                for r in range(phases):
                    power = [res_ref[q, p, r] for q in range(poles)]
                    for m in range(STEPS):
                        total = power[0]
                        for q in range(1, poles):
                            total = total + power[q]
                        coef[m, p * phases + r : p * phases + r + 1, :] = total
                        if m + 1 < STEPS:
                            power = [power[q] * pole_ref[q] for q in range(poles)]

    def build_history():
        for load in loads:
            load.wait()
        delay = delay_ref[...]

        def one(g, carry):
            first = pl.multiple_of(g * SUBLANES, SUBLANES)
            at = pl.ds(first, SUBLANES)

            def row(lead_index):
                return pl.ds(pl.multiple_of(lead_index * count + first, SUBLANES), SUBLANES)

            old = []
            for t in range(1, STEPS + 1):
                per_phase = []
                for r in range(phases):
                    value = jnp.zeros((SUBLANES, slots), jnp.float32)
                    for d in range(t, depth + 1):
                        value = jnp.where(delay == d, hist[row((d - t) * phases + r), :], value)
                    per_phase.append(value)
                old.append(per_phase)
            for p in range(phases):
                sums = [jnp.zeros((SUBLANES, slots), jnp.float32) for _ in range(STEPS)]
                for q in range(poles):
                    x = wave[row(q * phases + p), :]
                    y = admit[row(q * phases + p), :]
                    for t in range(STEPS):
                        x = x * polew_ref[q]
                        y = y * polea_ref[q]
                        sums[t] = sums[t] + (x - y)
                for t in range(STEPS):
                    for s in range(t + 1):
                        for r in range(phases):
                            k = p * phases + r
                            sums[t] = sums[t] + coef_w[t - s, k : k + 1, :] * old[s][r]
                    hist_sum[t, p, at, :] = sums[t]
            return carry

        lax.fori_loop(0, count // SUBLANES, one, 0)

    def build_packers():
        owner = lax.broadcasted_iota(jnp.int32, (devices, slots), 0)
        hits = as_hot((owner == partner_ref[...]) & (live_ref[...] > 0))
        before = as_hot(
            lax.broadcasted_iota(jnp.int32, (slots, slots), 0)
            < lax.broadcasted_iota(jnp.int32, (slots, slots), 1)
        )
        counts = dot_nn(hits, before) * hits.astype(jnp.float32)
        rank = jnp.sum(counts, axis=0, keepdims=True).astype(jnp.int32)
        stride = slots
        place = jnp.where(live_ref[...] > 0, partner_ref[...] * stride + rank, -1)
        if base:
            row = lax.broadcasted_iota(jnp.int32, (devices * base, slots), 0)
            pack_main[...] = as_hot((row // base) * stride + lax.rem(row, base) == place)
        row = lax.broadcasted_iota(jnp.int32, (devices * left, slots), 0)
        owner = row // left
        index = lax.rem(row, left)
        for k in range(groups + tiles):
            if k < groups:
                wanted = (index - spare) * groups + k
                fits = (index >= spare) & (wanted < capacity)
            else:
                wanted = base + index // tiles
                fits = (index < spare) & (lax.rem(index, tiles) == k - groups)
            wanted = jnp.where(fits, owner * stride + wanted, -2)
            pack_left[:, k * slots : (k + 1) * slots] = as_hot(wanted == place)

    def build_fault():
        same = lax.broadcasted_iota(jnp.int32, (count, count), 0) == lax.broadcasted_iota(
            jnp.int32, (count, count), 1
        )
        node = jnp.sum(jnp.where(same, fnode_ref[...].astype(jnp.float32), 0.0), axis=1, keepdims=True)
        strength = jnp.sum(jnp.where(same, fcond_ref[...], 0.0), axis=1, keepdims=True)
        local = node.astype(jnp.int32) - (net * nodes + line * width)
        lane = lax.broadcasted_iota(jnp.int32, (count, width), 1)
        fault[...] = jnp.where(lane == local, strength, 0.0)

    def swap(target, s):
        return remote(
            part.at[target, rows(s)], r1.at[target, rows(s)], a_send.at[target, s], a_recv.at[target, s], mate
        )

    def hop(side, target, s, i, to):
        return remote(
            mine.at[target, bits(s, i)], rbuf.at[side, target, bits(s, i)],
            b_send.at[target, s, i], b_recv.at[side, target, s, i], to,
        )

    def pass_on(target, s, i, right, left_way):
        @pl.when(right)
        def _():
            hop(0, target, s, i, line + CORES).start()

        @pl.when(left_way)
        def _():
            hop(1, target, s, i, line - CORES).start()

    def sum_finish(e, s):
        target = nearest(chips - 1 - e)
        swap(target, s).wait_recv()
        mine[target, rows(s)] = mine[target, rows(s)] + r1[target, rows(s)]
        for i in range(PIECES):
            pass_on(target, s, i, (z == 0) & (target > z), (z == chips - 1) & (target < z))

    def sum_compute(s):
        def one(e, carry):
            target = nearest(chips - 1 - e)

            def both(j, carry):
                got = spread(target * CORES + lax.rem(core + 1 + j, CORES), s)

                @pl.when(j == 0)
                def _():
                    part[target, rows(s)] = got
                    swap(target, s).start()

                @pl.when(j == 1)
                def _():
                    mine[target, rows(s)] = got

                return carry

            lax.fori_loop(0, CORES, both, 0)

            @pl.when(e > 0)
            def _():
                sum_finish(e - 1, s)

            return carry

        lax.fori_loop(0, chips, one, 0)
        sum_finish(chips - 1, s)

    def sum_relay(e, s):
        target = nearest(chips - 1 - e)

        def arrive(side, i):
            hop(side, target, s, i, mate).wait_recv()
            mine[target, bits(s, i)] = mine[target, bits(s, i)] + rbuf[side, target, bits(s, i)]

        for i in range(PIECES):
            @pl.when((target >= z) & (z > 0))
            def _():
                arrive(0, i)

            @pl.when((target <= z) & (z + 1 < chips))
            def _():
                arrive(1, i)

            pass_on(target, s, i, (target > z) & (z > 0), (target < z) & (z + 1 < chips))

    def sum_drain(s):
        def one(target, carry):
            swap(target, s).wait_send()

            @pl.when(target != z)
            def _():
                for i in range(PIECES):
                    hop(0, target, s, i, mate).wait_send()

            return carry

        lax.fori_loop(0, chips, one, 0)

    def exchange_copy(t, s, i):
        peer = lax.rem(me + 1 + i, devices)
        return pltpu.make_async_remote_copy(
            src_ref=xsend.at[s, peer], dst_ref=xrecv.at[t, s, me], send_sem=x_send.at[s, i],
            recv_sem=x_recv.at[t, s, i],
            device_id={"net": peer // lines, "line": lax.rem(peer, lines)}, device_id_type=MESH,
        )

    def exchange_start(t, s):
        surge = surge_ref[...]
        live = live_ref[...].astype(jnp.float32)
        wave_out = jnp.concatenate(
            [(2.0 * surge * ends[p, rows(s)] - h[p, rows(s)]) * live for p in range(phases)], axis=0
        )
        high, low = split_two(wave_out)
        body = tiles * LANES
        if base:
            main = dot_nt(pack_main[...], jnp.concatenate([high[:body], low[:body]], axis=0))
            main = main[:, :body] + main[:, body:]
            for j in range(tiles):
                xsend[s, :, j * base : (j + 1) * base, :] = main[:, j * LANES : (j + 1) * LANES].reshape(
                    devices, base, LANES
                )
        for offset, value in ((0, high), (LANES, low)):
            for k in range(groups):
                left_rhs[offset + k * rest : offset + (k + 1) * rest, k * slots : (k + 1) * slots] = value[body:]
            for j in range(tiles):
                left_rhs[offset : offset + LANES, (groups + j) * slots : (groups + j + 1) * slots] = value[
                    j * LANES : (j + 1) * LANES
                ]
        tail = dot_nt(pack_left[...], left_rhs[...])
        tail = tail[:, :LANES] + tail[:, LANES:]
        xsend[s, :, lead : lead + left, :] = tail.reshape(devices, left, LANES)

        def go(i, carry):
            exchange_copy(t, s, i).start()
            return carry

        lax.fori_loop(0, devices - 1, go, 0)

    def exchange_finish(t, s):
        def end(i, carry):
            exchange_copy(t, s, i).wait()
            return carry

        lax.fori_loop(0, devices - 1, end, 0)

    def unpack(t, s):
        tail = xrecv[t, s, :, lead : lead + left, :].reshape(devices * left, LANES).T
        high, low = split_two(tail)
        arrived = []
        if base:
            for j in range(tiles):
                main = xrecv[t, s, :, j * base : (j + 1) * base, :].reshape(devices * base, LANES).T
                arrived.append(fold_two(dot_nn(stack_two(main), pack_main[...])))
        for j in range(tiles):
            k = groups + j
            more = fold_two(
                dot_nn(jnp.concatenate([high, low], axis=0), pack_left[:, k * slots : (k + 1) * slots])
            )
            if base:
                arrived[j] = arrived[j] + more
            else:
                arrived.append(more)
        last = jnp.zeros((rest, slots), jnp.float32)
        for k in range(groups):
            here = slice(k * rest, (k + 1) * rest)
            last = last + fold_two(
                dot_nn(jnp.concatenate([high[here], low[here]], axis=0), pack_left[:, k * slots : (k + 1) * slots])
            )
        return jnp.concatenate(arrived + [last], axis=0)

    def mixed(coef, m, p, values):
        total = coef[m, p * phases : p * phases + 1, :] * values[0]
        for r in range(1, phases):
            total = total + coef[m, p * phases + r : p * phases + r + 1, :] * values[r]
        return total

    def add_ends(t, s):
        values = [ends[r, rows(s)] for r in range(phases)]
        for m in range(STEPS):
            @pl.when(t + m < STEPS)
            def _():
                for p in range(phases):
                    hist_sum[t + m, p, rows(s)] = hist_sum[t + m, p, rows(s)] - mixed(coef_a, m, p, values)

    def add_waves(t, s):
        arrived = unpack(t - 1, s)
        delay = delay_ref[...]
        for d in range(1, STEPS):
            values = [
                jnp.where(delay == d, arrived[r * half : (r + 1) * half], 0.0) for r in range(phases)
            ]
            for m in range(STEPS - d):
                @pl.when(t + d - 1 + m < STEPS)
                def _():
                    for p in range(phases):
                        at = t + d - 1 + m
                        hist_sum[at, p, rows(s)] = hist_sum[at, p, rows(s)] + mixed(coef_w, m, p, values)

    left_rhs[...] = jnp.zeros_like(left_rhs)
    build_coef()
    build_fault()
    pl.semaphore_wait(barrier, devices - 1)
    isems = (ic_send, ic_recv, id_send, id_recv)
    vsems = (vc_send, vc_recv, vd_send, vd_recv)
    for s in range(SPLIT):
        gather_start(vfull, vsems, s)
    ends[...] = jnp.zeros_like(ends)
    build_hot()

    def first(e, carry):
        gather_arrive(vfull, vsems, 0, e)

        @pl.when(e == 1)
        def _():
            if turned:
                build_hot_t()

        @pl.when(e == 2)
        def _():
            build_history()
            for block in range(lines):
                stage(block).start()

        gather_take(vfull, vsems, 0, e, pick)
        return carry

    lax.fori_loop(0, chips, first, 0)
    gather_last(vfull, vsems, 0, pick)
    gather_drain(vfull, vsems, 0)
    add_ends(0, 0)

    def run_half(k, carry):
        s = lax.rem(k, SPLIT)
        o = 1 - s
        t = k // SPLIT
        done = t + s

        @pl.when(t > 0)
        def _():
            exchange_finish(t - 1, s)
            add_waves(t, s)

        live = live_ref[...].astype(jnp.float32)
        for p in range(phases):
            now = hist_sum[t, p, rows(s)] * live
            h[p, rows(s)] = now
            h_split[p] = stack_two(now)
        sum_compute(s)

        @pl.when(k == 0)
        def _():
            build_inverse()

        @pl.when(k > 0)
        def _():
            ends[:, rows(o)] = jnp.zeros_like(ends[:, rows(o)])

        def merged(e, carry):
            gather_arrive(vfull, vsems, o, e)
            sum_relay(e, s)
            gather_take(vfull, vsems, o, e, pick)
            return carry

        lax.fori_loop(0, chips, merged, 0)
        ifull[line, rows(s)] = mine[z, rows(s)] + (source_ref[t] - fault[rows(s)] * vfull[line, rows(s)])
        gather_start(ifull, isems, s)
        gather_last(vfull, vsems, o, pick)
        gather_drain(vfull, vsems, o)

        @pl.when(k == 0)
        def _():
            build_packers()

        @pl.when((done > 0) & (done < STEPS))
        def _():
            exchange_start(done - 1, o)

        @pl.when(done < STEPS)
        def _():
            add_ends(done, o)

        volt_ref[rows(s)] = jnp.zeros_like(volt_ref[rows(s)])

        def answer(e, carry):
            gather_arrive(ifull, isems, s, e)
            gather_take(ifull, isems, s, e, solve)
            return carry

        lax.fori_loop(0, chips, answer, 0)
        gather_last(ifull, isems, s, solve)
        vfull[line, rows(s)] = volt_ref[rows(s)]
        gather_start(vfull, vsems, s)
        gather_drain(ifull, isems, s)
        sum_drain(s)
        return carry

    lax.fori_loop(0, SPLIT * STEPS, run_half, 0)
    o = SPLIT - 1
    ends[:, rows(o)] = jnp.zeros_like(ends[:, rows(o)])

    def final(e, carry):
        gather_arrive(vfull, vsems, o, e)
        gather_take(vfull, vsems, o, e, pick)
        return carry

    lax.fori_loop(0, chips, final, 0)
    gather_last(vfull, vsems, o, pick)
    live = live_ref[...].astype(jnp.float32)
    for p in range(phases):
        curr_ref[p] = (surge_ref[...] * ends[p] - h[p]) * live
    gather_drain(vfull, vsems, o)


def hand_over(volt_ref, curr_ref, volt_out, curr_out):
    volt_out[...] = volt_ref[...]
    curr_out[...] = curr_ref[...]


def on_device(
    conductance_inverse, prior_voltage, sources, fault_node, fault_conductance, terminal_node,
    ownership, partner, delay_steps, surge_conductance, pole_wave, residue_wave, pole_admit,
    residue_admit, wave_state, admit_state, wave_history,
):
    lines = lax.axis_size("line")
    nets = lax.axis_size("net")
    devices = lines * nets
    chips = lines // CORES
    inverse = conductance_inverse[0]
    prior = prior_voltage[0]
    terminal = terminal_node[0]
    count, width = prior.shape
    phases, slots = terminal.shape
    wave = wave_state.reshape(-1, slots)
    admit = admit_state.reshape(-1, slots)
    hist = wave_history.reshape(-1, slots)
    capacity = (slots + devices - 2) // (devices - 1)
    half = count // SPLIT
    tiles, rest, groups, base, spare, left = message_plan(capacity, phases * half)
    message = tiles * base + left
    turned = devices * left <= slots
    f32, bf16 = jnp.float32, jnp.bfloat16
    vmem = lambda: pl.BlockSpec(memory_space=pltpu.VMEM)
    hbm = lambda: pl.BlockSpec(memory_space=pltpu.HBM)
    dma = lambda *shape: pltpu.SemaphoreType.DMA(shape)
    gather_sems = [
        dma(2, chips, SPLIT, PIECES), dma(chips, SPLIT, PIECES), dma(chips, SPLIT), dma(chips, SPLIT),
    ]
    volt, curr = pl.pallas_call(
        functools.partial(kernel, lines, nets),
        out_shape=(
            jax.ShapeDtypeStruct((count, width), f32),
            jax.ShapeDtypeStruct((phases, count, slots), f32),
        ),
        in_specs=[vmem()] * 13 + [hbm()] * 4,
        out_specs=(vmem(), vmem()),
        scratch_shapes=[
            pltpu.VMEM(wave.shape, f32),
            pltpu.VMEM(admit.shape, f32),
            pltpu.VMEM(hist.shape, f32),
            pltpu.VMEM((lines, inverse.shape[0], width), bf16),
            pltpu.VMEM((lines, inverse.shape[0], width), bf16),
            pltpu.VMEM((phases, lines, width, slots), bf16),
            pltpu.VMEM((phases, lines, slots, width) if turned else (SUBLANES, LANES), bf16),
            pltpu.VMEM((devices * max(base, SUBLANES), slots), bf16),
            pltpu.VMEM((devices * left, (groups + tiles) * slots), bf16),
            pltpu.VMEM((2 * LANES, (groups + tiles) * slots), bf16),
            pltpu.VMEM((STEPS, phases * phases, slots), f32),
            pltpu.VMEM((STEPS, phases * phases, slots), f32),
            pltpu.VMEM((STEPS, phases, count, slots), f32),
            pltpu.VMEM((phases, count, slots), f32),
            pltpu.VMEM((phases, count, slots), f32),
            pltpu.VMEM((phases, 2 * half, slots), bf16),
            pltpu.VMEM((count, width), f32),
            pltpu.VMEM((lines, count, width), f32),
            pltpu.VMEM((lines, count, width), f32),
            pltpu.VMEM((chips, count, width), f32),
            pltpu.VMEM((chips, count, width), f32),
            pltpu.VMEM((chips, count, width), f32),
            pltpu.VMEM((2, chips, count, width), f32),
            pltpu.VMEM((SPLIT, devices, message, LANES), f32),
            pltpu.VMEM((STEPS - 1, SPLIT, devices, message, LANES), f32),
            dma(3), dma(lines), dma(chips, SPLIT), dma(chips, SPLIT), dma(chips, SPLIT, PIECES), dma(2, chips, SPLIT, PIECES),
        ] + gather_sems + gather_sems + [dma(SPLIT, devices), dma(STEPS - 1, SPLIT, devices)],
        compiler_params=pltpu.CompilerParams(
            collective_id=0, has_side_effects=True, vmem_limit_bytes=67043328
        ),
        name="network",
    )(
        prior, sources, fault_node[None], fault_conductance[None], terminal[:, None], ownership, partner,
        delay_steps, surge_conductance, pole_wave[0][:, None], residue_wave[0][:, :, :, None],
        pole_admit[0][:, None], residue_admit[0][:, :, :, None],
        inverse, wave, admit, hist,
    )
    volt, curr = pl.pallas_call(
        hand_over,
        out_shape=(jax.ShapeDtypeStruct(volt.shape, f32), jax.ShapeDtypeStruct(curr.shape, f32)),
        in_specs=[vmem(), vmem()],
        out_specs=(vmem(), vmem()),
        name="hand_over",
    )(volt, curr)
    return volt[None], curr[None]


def solution(mesh):
    return jax.shard_map(
        on_device,
        mesh=mesh,
        in_specs=(
            P("net", "line", None),
            P("net", None, "line"),
            P(None, "net", "line"),
            P(),
            P(),
            P("net", None, "line"),
            P("net", "line"),
            P("net", "line"),
            P("net", "line"),
            P("net", "line"),
            P("net", None, "line"),
            P("net", None, None, None, "line"),
            P("net", None, "line"),
            P("net", None, None, None, "line"),
            P("net", None, None, None, "line"),
            P("net", None, None, None, "line"),
            P("net", None, None, None, "line"),
        ),
        out_specs=(P("net", None, "line"), P("net", None, None, "line")),
        check_vma=False,
    )
```

```python
import functools

import jax
import jax.numpy as jnp
from jax import lax
from jax.experimental import pallas as pl
from jax.experimental.pallas import tpu as pltpu
from jax.sharding import PartitionSpec as P

STEPS = 3
CORES = 2
SPLIT = 2
PIECES = 3
LANES = 128
SUBLANES = 8
MESH = pl.DeviceIdType.MESH


def split_two(value):
    high = value.astype(jnp.bfloat16)
    low = (value - high.astype(jnp.float32)).astype(jnp.bfloat16)
    return high, low


def stack_two(value):
    return jnp.concatenate(split_two(value), axis=0)


def fold_two(value):
    half = value.shape[0] // 2
    return value[:half] + value[half:]


def dot_nt(left, right):
    return lax.dot_general(left, right, (((1,), (1,)), ((), ())), preferred_element_type=jnp.float32)


def dot_nn(left, right):
    return lax.dot_general(left, right, (((1,), (0,)), ((), ())), preferred_element_type=jnp.float32)


def as_hot(mask):
    return mask.astype(jnp.float32).astype(jnp.bfloat16)


def message_plan(capacity, width):
    tiles, rest = width // LANES, width % LANES
    groups = LANES // rest
    base = capacity // SUBLANES * SUBLANES
    spare = (capacity - base) * tiles
    left = -(-(spare + -(-capacity // groups)) // SUBLANES) * SUBLANES
    return tiles, rest, groups, base, spare, left


def kernel(
    lines, nets,
    prior_ref, source_ref, fnode_ref, fcond_ref, term_ref, live_ref, partner_ref, delay_ref, surge_ref,
    polew_ref, resw_ref, polea_ref, resa_ref, inv_hbm, wave_hbm, admit_hbm, hist_hbm,
    volt_ref, curr_ref,
    wave, admit, hist, inv_high, inv_low, hot, hot_t, pack_main, pack_left, left_rhs,
    coef_w, coef_a, hist_sum, ends, h, h_split, fault, ifull, vfull,
    part, r1, mine, rbuf, xsend, xrecv,
    load_sem, inv_sem, a_send, a_recv, b_send, b_recv,
    ic_send, ic_recv, id_send, id_recv, vc_send, vc_recv, vd_send, vd_recv, x_send, x_recv,
):
    chips = lines // CORES
    devices = lines * nets
    net = lax.axis_index("net")
    line = lax.axis_index("line")
    z = line // CORES
    core = lax.rem(line, CORES)
    me = net * lines + line
    mate = z * CORES + 1 - core
    phases, count, slots = h.shape
    width = ifull.shape[2]
    nodes = width * lines
    half = count // SPLIT
    piece = half // PIECES
    poles = polew_ref.shape[0]
    depth = hist.shape[0] // (phases * count)
    capacity = (slots + devices - 2) // (devices - 1)
    tiles, rest, groups, base, spare, left = message_plan(capacity, phases * half)
    lead = tiles * base
    turned = len(hot_t.shape) == 4
    used = lead + spare + -(-capacity // groups)

    def remote(src, dst, send, recv, target):
        return pltpu.make_async_remote_copy(
            src_ref=src, dst_ref=dst, send_sem=send, recv_sem=recv,
            device_id={"line": target}, device_id_type=MESH,
        )

    def nearest(e):
        near = jnp.minimum(z, chips - 1 - z)
        both = jnp.where(lax.rem(e, 2) == 1, z - (e + 1) // 2, z + e // 2)
        one = jnp.where(z > near, z - (e - near), z + (e - near))
        return jnp.where(e <= 2 * near, both, one)

    def rows(s):
        return pl.ds(pl.multiple_of(s * half, half), half)

    def bits(s, i):
        return pl.ds(pl.multiple_of(s * half + i * piece, piece), piece)

    states = ((wave_hbm, wave), (admit_hbm, admit), (hist_hbm, hist))
    loads = [pltpu.make_async_copy(src, dst, load_sem.at[i]) for i, (src, dst) in enumerate(states)]
    for load in loads:
        load.start()

    places = [(dst, at) for _, dst in states for at in range(0, dst.shape[0] - width + 1, width)][:lines]

    def stage(block):
        dst, at = places[block]
        return pltpu.make_async_copy(
            inv_hbm.at[:, pl.ds(block * width, width)], dst.at[pl.ds(at, width), pl.ds(0, width)],
            inv_sem.at[block],
        )

    xrecv[...] = jnp.zeros_like(xrecv)
    barrier = pltpu.get_barrier_semaphore()

    def greet(i, carry):
        peer = lax.rem(me + 1 + i, devices)
        pl.semaphore_signal(
            barrier, inc=1, device_id={"net": peer // lines, "line": lax.rem(peer, lines)},
            device_id_type=MESH,
        )
        return carry

    lax.fori_loop(0, devices - 1, greet, 0)
    vfull[line] = prior_ref[...]

    def gather_hop(buf, sems, block, source, s, i, side, to):
        view = buf.at[block, bits(s, i)]
        return remote(view, view, sems[0].at[side, source, s, i], sems[1].at[source, s, i], to)

    def gather_start(buf, sems, s):
        c_send, c_recv, d_send, d_recv = sems

        @pl.when(z + 1 < chips)
        def _():
            for i in range(PIECES):
                gather_hop(buf, sems, line, z, s, i, 0, line + CORES).start()

        @pl.when(z > 0)
        def _():
            for i in range(PIECES):
                gather_hop(buf, sems, line, z, s, i, 1, line - CORES).start()

        view = buf.at[line, rows(s)]
        remote(view, view, d_send.at[z, s], d_recv.at[z, s], mate).start()

    def gather_arrive(buf, sems, s, e):
        c_send, c_recv, d_send, d_recv = sems
        source = nearest(e)
        block = source * CORES + core

        @pl.when(e > 0)
        def _():
            for i in range(PIECES):
                gather_hop(buf, sems, block, source, s, i, 0, mate).wait_recv()

                @pl.when((source < z) & (z + 1 < chips))
                def _():
                    gather_hop(buf, sems, block, source, s, i, 0, line + CORES).start()

                @pl.when((source > z) & (z > 0))
                def _():
                    gather_hop(buf, sems, block, source, s, i, 1, line - CORES).start()

            view = buf.at[block, rows(s)]
            remote(view, view, d_send.at[source, s], d_recv.at[source, s], mate).start()

    def gather_take(buf, sems, s, e, consume):
        c_send, c_recv, d_send, d_recv = sems

        def take(j, carry):
            source = nearest(jnp.maximum(e - j, 0))

            @pl.when((e < chips) & (j == 0))
            def _():
                consume(source * CORES + core, s)

            @pl.when((e > 0) & (j == 1))
            def _():
                view = buf.at[source * CORES + 1 - core, rows(s)]
                remote(view, view, d_send.at[source, s], d_recv.at[source, s], mate).wait_recv()
                consume(source * CORES + 1 - core, s)

            return carry

        lax.fori_loop(0, CORES, take, 0)

    def gather_last(buf, sems, s, consume):
        source = nearest(chips - 1)
        view = buf.at[source * CORES + 1 - core, rows(s)]
        remote(view, view, sems[2].at[source, s], sems[3].at[source, s], mate).wait_recv()
        consume(source * CORES + 1 - core, s)

    def gather_drain(buf, sems, s):
        c_send, c_recv, d_send, d_recv = sems

        def drain(source, carry):
            block = source * CORES + core
            view = buf.at[block, rows(s)]
            remote(view, view, d_send.at[source, s], d_recv.at[source, s], mate).wait_send()

            @pl.when((source <= z) & (z + 1 < chips))
            def _():
                for i in range(PIECES):
                    gather_hop(buf, sems, block, source, s, i, 0, mate).wait_send()

            @pl.when((source >= z) & (z > 0))
            def _():
                for i in range(PIECES):
                    gather_hop(buf, sems, block, source, s, i, 1, mate).wait_send()

            return carry

        lax.fori_loop(0, chips, drain, 0)

    def pick(block, s):
        both = stack_two(vfull[block, rows(s)])
        for p in range(phases):
            ends[p, rows(s)] += fold_two(dot_nn(both, hot[p, block]))

    def spread(block, s):
        total = jnp.zeros((half, width), jnp.float32)
        for p in range(phases):
            if turned:
                total = total + fold_two(dot_nn(h_split[p], hot_t[p, block]))
            else:
                total = total + fold_two(dot_nt(h_split[p], hot[p, block]))
        return total

    def solve(block, s):
        both = stack_two(ifull[block, rows(s)])
        got = dot_nn(both, inv_high[block])
        volt_ref[rows(s)] += got[:half] + (got[half:] + dot_nn(both[:half], inv_low[block]))

    def build_hot():
        def one(block, carry):
            lane = lax.broadcasted_iota(jnp.int32, (width, slots), 0) + block * width
            for p in range(phases):
                hot[p, block] = as_hot(lane == term_ref[p])
            return carry

        lax.fori_loop(0, lines, one, 0)

    def build_hot_t():
        for p in range(phases):
            tall = jnp.broadcast_to(term_ref[p].astype(jnp.float32), (LANES, slots)).T.astype(jnp.int32)
            lane = lax.broadcasted_iota(jnp.int32, (slots, LANES), 1)

            def one(block, carry):
                for j in range(width // LANES):
                    hot_t[p, block, :, j * LANES : (j + 1) * LANES] = as_hot(
                        lane + (block * width + j * LANES) == tall
                    )
                return carry

            lax.fori_loop(0, lines, one, 0)

    def build_inverse():
        for block in range(lines):
            dst, at = places[block]
            stage(block).wait()
            high, low = split_two(dst[pl.ds(at, width), :width].T)
            inv_high[block] = high
            inv_low[block] = low

    def build_coef():
        for pole_ref, res_ref, coef in ((polew_ref, resw_ref, coef_w), (polea_ref, resa_ref, coef_a)):
            for p in range(phases):
                for r in range(phases):
                    power = [res_ref[q, p, r] for q in range(poles)]
                    for m in range(STEPS):
                        total = power[0]
                        for q in range(1, poles):
                            total = total + power[q]
                        coef[m, p * phases + r : p * phases + r + 1, :] = total
                        if m + 1 < STEPS:
                            power = [power[q] * pole_ref[q] for q in range(poles)]

    def build_history():
        for load in loads:
            load.wait()
        delay = delay_ref[...]

        def one(g, carry):
            first = pl.multiple_of(g * SUBLANES, SUBLANES)
            at = pl.ds(first, SUBLANES)

            def row(lead_index):
                return pl.ds(pl.multiple_of(lead_index * count + first, SUBLANES), SUBLANES)

            old = []
            for t in range(1, STEPS + 1):
                per_phase = []
                for r in range(phases):
                    value = jnp.zeros((SUBLANES, slots), jnp.float32)
                    for d in range(t, depth + 1):
                        value = jnp.where(delay == d, hist[row((d - t) * phases + r), :], value)
                    per_phase.append(value)
                old.append(per_phase)
            for p in range(phases):
                sums = [jnp.zeros((SUBLANES, slots), jnp.float32) for _ in range(STEPS)]
                for q in range(poles):
                    x = wave[row(q * phases + p), :]
                    y = admit[row(q * phases + p), :]
                    for t in range(STEPS):
                        x = x * polew_ref[q]
                        y = y * polea_ref[q]
                        sums[t] = sums[t] + (x - y)
                for t in range(STEPS):
                    for s in range(t + 1):
                        for r in range(phases):
                            k = p * phases + r
                            sums[t] = sums[t] + coef_w[t - s, k : k + 1, :] * old[s][r]
                    hist_sum[t, p, at, :] = sums[t]
            return carry

        lax.fori_loop(0, count // SUBLANES, one, 0)

    def build_packers():
        owner = lax.broadcasted_iota(jnp.int32, (devices, slots), 0)
        hits = as_hot((owner == partner_ref[...]) & (live_ref[...] > 0))
        before = as_hot(
            lax.broadcasted_iota(jnp.int32, (slots, slots), 0)
            < lax.broadcasted_iota(jnp.int32, (slots, slots), 1)
        )
        counts = dot_nn(hits, before) * hits.astype(jnp.float32)
        rank = jnp.sum(counts, axis=0, keepdims=True).astype(jnp.int32)
        stride = slots
        place = jnp.where(live_ref[...] > 0, partner_ref[...] * stride + rank, -1)
        if base:
            row = lax.broadcasted_iota(jnp.int32, (devices * base, slots), 0)
            pack_main[...] = as_hot((row // base) * stride + lax.rem(row, base) == place)
        row = lax.broadcasted_iota(jnp.int32, (devices * left, slots), 0)
        owner = row // left
        index = lax.rem(row, left)
        for k in range(groups + tiles):
            if k < groups:
                wanted = (index - spare) * groups + k
                fits = (index >= spare) & (wanted < capacity)
            else:
                wanted = base + index // tiles
                fits = (index < spare) & (lax.rem(index, tiles) == k - groups)
            wanted = jnp.where(fits, owner * stride + wanted, -2)
            pack_left[:, k * slots : (k + 1) * slots] = as_hot(wanted == place)

    def build_fault():
        same = lax.broadcasted_iota(jnp.int32, (count, count), 0) == lax.broadcasted_iota(
            jnp.int32, (count, count), 1
        )
        node = jnp.sum(jnp.where(same, fnode_ref[...].astype(jnp.float32), 0.0), axis=1, keepdims=True)
        strength = jnp.sum(jnp.where(same, fcond_ref[...], 0.0), axis=1, keepdims=True)
        local = node.astype(jnp.int32) - (net * nodes + line * width)
        lane = lax.broadcasted_iota(jnp.int32, (count, width), 1)
        fault[...] = jnp.where(lane == local, strength, 0.0)

    def swap(target, s):
        return remote(
            part.at[target, rows(s)], r1.at[target, rows(s)], a_send.at[target, s], a_recv.at[target, s], mate
        )

    def hop(side, target, s, i, to):
        return remote(
            mine.at[target, bits(s, i)], rbuf.at[side, target, bits(s, i)],
            b_send.at[target, s, i], b_recv.at[side, target, s, i], to,
        )

    def pass_on(target, s, i, right, left_way):
        @pl.when(right)
        def _():
            hop(0, target, s, i, line + CORES).start()

        @pl.when(left_way)
        def _():
            hop(1, target, s, i, line - CORES).start()

    def sum_finish(e, s):
        target = nearest(chips - 1 - e)
        swap(target, s).wait_recv()
        mine[target, rows(s)] = mine[target, rows(s)] + r1[target, rows(s)]
        for i in range(PIECES):
            pass_on(target, s, i, (z == 0) & (target > z), (z == chips - 1) & (target < z))

    def sum_compute(s):
        def one(e, carry):
            target = nearest(chips - 1 - e)

            def both(j, carry):
                got = spread(target * CORES + lax.rem(core + 1 + j, CORES), s)

                @pl.when(j == 0)
                def _():
                    part[target, rows(s)] = got
                    swap(target, s).start()

                @pl.when(j == 1)
                def _():
                    mine[target, rows(s)] = got

                return carry

            lax.fori_loop(0, CORES, both, 0)

            @pl.when(e > 0)
            def _():
                sum_finish(e - 1, s)

            return carry

        lax.fori_loop(0, chips, one, 0)
        sum_finish(chips - 1, s)

    def sum_relay(e, s):
        target = nearest(chips - 1 - e)

        def arrive(side, i):
            hop(side, target, s, i, mate).wait_recv()
            mine[target, bits(s, i)] = mine[target, bits(s, i)] + rbuf[side, target, bits(s, i)]

        for i in range(PIECES):
            @pl.when((target >= z) & (z > 0))
            def _():
                arrive(0, i)

            @pl.when((target <= z) & (z + 1 < chips))
            def _():
                arrive(1, i)

            pass_on(target, s, i, (target > z) & (z > 0), (target < z) & (z + 1 < chips))

    def sum_drain(s):
        def one(target, carry):
            swap(target, s).wait_send()

            @pl.when(target != z)
            def _():
                for i in range(PIECES):
                    hop(0, target, s, i, mate).wait_send()

            return carry

        lax.fori_loop(0, chips, one, 0)

    def exchange_copy(t, s, i):
        peer = lax.rem(me + 1 + i, devices)
        return pltpu.make_async_remote_copy(
            src_ref=xsend.at[s, peer, pl.ds(0, used)], dst_ref=xrecv.at[t, s, me, pl.ds(0, used)], send_sem=x_send.at[s, i],
            recv_sem=x_recv.at[t, s, i],
            device_id={"net": peer // lines, "line": lax.rem(peer, lines)}, device_id_type=MESH,
        )

    def exchange_start(t, s):
        surge = surge_ref[...]
        live = live_ref[...].astype(jnp.float32)
        wave_out = jnp.concatenate(
            [(2.0 * surge * ends[p, rows(s)] - h[p, rows(s)]) * live for p in range(phases)], axis=0
        )
        high, low = split_two(wave_out)
        body = tiles * LANES
        if base:
            main = dot_nt(pack_main[...], jnp.concatenate([high[:body], low[:body]], axis=0))
            main = main[:, :body] + main[:, body:]
            for j in range(tiles):
                xsend[s, :, j * base : (j + 1) * base, :] = main[:, j * LANES : (j + 1) * LANES].reshape(
                    devices, base, LANES
                )
        for offset, value in ((0, high), (LANES, low)):
            for k in range(groups):
                left_rhs[offset + k * rest : offset + (k + 1) * rest, k * slots : (k + 1) * slots] = value[body:]
            for j in range(tiles):
                left_rhs[offset : offset + LANES, (groups + j) * slots : (groups + j + 1) * slots] = value[
                    j * LANES : (j + 1) * LANES
                ]
        tail = dot_nt(pack_left[...], left_rhs[...])
        tail = tail[:, :LANES] + tail[:, LANES:]
        xsend[s, :, lead : lead + left, :] = tail.reshape(devices, left, LANES)

        def go(i, carry):
            exchange_copy(t, s, i).start()
            return carry

        lax.fori_loop(0, devices - 1, go, 0)

    def exchange_finish(t, s):
        def end(i, carry):
            exchange_copy(t, s, i).wait()
            return carry

        lax.fori_loop(0, devices - 1, end, 0)

    def unpack(t, s):
        tail = xrecv[t, s, :, lead : lead + left, :].reshape(devices * left, LANES).T
        high, low = split_two(tail)
        arrived = []
        if base:
            for j in range(tiles):
                main = xrecv[t, s, :, j * base : (j + 1) * base, :].reshape(devices * base, LANES).T
                arrived.append(fold_two(dot_nn(stack_two(main), pack_main[...])))
        for j in range(tiles):
            k = groups + j
            more = fold_two(
                dot_nn(jnp.concatenate([high, low], axis=0), pack_left[:, k * slots : (k + 1) * slots])
            )
            if base:
                arrived[j] = arrived[j] + more
            else:
                arrived.append(more)
        last = jnp.zeros((rest, slots), jnp.float32)
        for k in range(groups):
            here = slice(k * rest, (k + 1) * rest)
            last = last + fold_two(
                dot_nn(jnp.concatenate([high[here], low[here]], axis=0), pack_left[:, k * slots : (k + 1) * slots])
            )
        return jnp.concatenate(arrived + [last], axis=0)

    def mixed(coef, m, p, values):
        total = coef[m, p * phases : p * phases + 1, :] * values[0]
        for r in range(1, phases):
            total = total + coef[m, p * phases + r : p * phases + r + 1, :] * values[r]
        return total

    def add_ends(t, s):
        values = [ends[r, rows(s)] for r in range(phases)]
        for m in range(STEPS):
            @pl.when(t + m < STEPS)
            def _():
                for p in range(phases):
                    hist_sum[t + m, p, rows(s)] = hist_sum[t + m, p, rows(s)] - mixed(coef_a, m, p, values)

    def add_waves(t, s):
        arrived = unpack(t - 1, s)
        delay = delay_ref[...]
        for d in range(1, STEPS):
            values = [
                jnp.where(delay == d, arrived[r * half : (r + 1) * half], 0.0) for r in range(phases)
            ]
            for m in range(STEPS - d):
                @pl.when(t + d - 1 + m < STEPS)
                def _():
                    for p in range(phases):
                        at = t + d - 1 + m
                        hist_sum[at, p, rows(s)] = hist_sum[at, p, rows(s)] + mixed(coef_w, m, p, values)

    left_rhs[...] = jnp.zeros_like(left_rhs)
    build_coef()
    build_fault()
    pl.semaphore_wait(barrier, devices - 1)
    isems = (ic_send, ic_recv, id_send, id_recv)
    vsems = (vc_send, vc_recv, vd_send, vd_recv)
    for s in range(SPLIT):
        gather_start(vfull, vsems, s)
    ends[...] = jnp.zeros_like(ends)
    build_hot()

    def first(e, carry):
        gather_arrive(vfull, vsems, 0, e)

        @pl.when(e == 1)
        def _():
            if turned:
                build_hot_t()

        @pl.when(e == 2)
        def _():
            build_history()
            for block in range(lines):
                stage(block).start()

        gather_take(vfull, vsems, 0, e, pick)
        return carry

    lax.fori_loop(0, chips, first, 0)
    gather_last(vfull, vsems, 0, pick)
    gather_drain(vfull, vsems, 0)
    add_ends(0, 0)

    def run_half(k, carry):
        s = lax.rem(k, SPLIT)
        o = 1 - s
        t = k // SPLIT
        done = t + s

        @pl.when(t > 0)
        def _():
            exchange_finish(t - 1, s)
            add_waves(t, s)

        live = live_ref[...].astype(jnp.float32)
        for p in range(phases):
            now = hist_sum[t, p, rows(s)] * live
            h[p, rows(s)] = now
            h_split[p] = stack_two(now)
        sum_compute(s)

        @pl.when(k == 0)
        def _():
            build_inverse()

        @pl.when(k > 0)
        def _():
            ends[:, rows(o)] = jnp.zeros_like(ends[:, rows(o)])

        def merged(e, carry):
            gather_arrive(vfull, vsems, o, e)
            sum_relay(e, s)
            gather_take(vfull, vsems, o, e, pick)
            return carry

        lax.fori_loop(0, chips, merged, 0)
        ifull[line, rows(s)] = mine[z, rows(s)] + (source_ref[t] - fault[rows(s)] * vfull[line, rows(s)])
        gather_start(ifull, isems, s)
        gather_last(vfull, vsems, o, pick)
        gather_drain(vfull, vsems, o)

        @pl.when(k == 0)
        def _():
            build_packers()

        @pl.when((done > 0) & (done < STEPS))
        def _():
            exchange_start(done - 1, o)

        @pl.when(done < STEPS)
        def _():
            add_ends(done, o)

        volt_ref[rows(s)] = jnp.zeros_like(volt_ref[rows(s)])

        def answer(e, carry):
            gather_arrive(ifull, isems, s, e)
            gather_take(ifull, isems, s, e, solve)
            return carry

        lax.fori_loop(0, chips, answer, 0)
        gather_last(ifull, isems, s, solve)
        vfull[line, rows(s)] = volt_ref[rows(s)]
        gather_start(vfull, vsems, s)
        gather_drain(ifull, isems, s)
        sum_drain(s)
        return carry

    lax.fori_loop(0, SPLIT * STEPS, run_half, 0)
    o = SPLIT - 1
    ends[:, rows(o)] = jnp.zeros_like(ends[:, rows(o)])

    def final(e, carry):
        gather_arrive(vfull, vsems, o, e)
        gather_take(vfull, vsems, o, e, pick)
        return carry

    lax.fori_loop(0, chips, final, 0)
    gather_last(vfull, vsems, o, pick)
    live = live_ref[...].astype(jnp.float32)
    for p in range(phases):
        curr_ref[p] = (surge_ref[...] * ends[p] - h[p]) * live
    gather_drain(vfull, vsems, o)


def hand_over(volt_ref, curr_ref, volt_out, curr_out):
    volt_out[...] = volt_ref[...]
    curr_out[...] = curr_ref[...]


def on_device(
    conductance_inverse, prior_voltage, sources, fault_node, fault_conductance, terminal_node,
    ownership, partner, delay_steps, surge_conductance, pole_wave, residue_wave, pole_admit,
    residue_admit, wave_state, admit_state, wave_history,
):
    lines = lax.axis_size("line")
    nets = lax.axis_size("net")
    devices = lines * nets
    chips = lines // CORES
    inverse = conductance_inverse[0]
    prior = prior_voltage[0]
    terminal = terminal_node[0]
    count, width = prior.shape
    phases, slots = terminal.shape
    wave = wave_state.reshape(-1, slots)
    admit = admit_state.reshape(-1, slots)
    hist = wave_history.reshape(-1, slots)
    capacity = (slots + devices - 2) // (devices - 1)
    half = count // SPLIT
    tiles, rest, groups, base, spare, left = message_plan(capacity, phases * half)
    message = tiles * base + left
    turned = devices * left <= slots
    f32, bf16 = jnp.float32, jnp.bfloat16
    vmem = lambda: pl.BlockSpec(memory_space=pltpu.VMEM)
    hbm = lambda: pl.BlockSpec(memory_space=pltpu.HBM)
    dma = lambda *shape: pltpu.SemaphoreType.DMA(shape)
    gather_sems = [
        dma(2, chips, SPLIT, PIECES), dma(chips, SPLIT, PIECES), dma(chips, SPLIT), dma(chips, SPLIT),
    ]
    volt, curr = pl.pallas_call(
        functools.partial(kernel, lines, nets),
        out_shape=(
            jax.ShapeDtypeStruct((count, width), f32),
            jax.ShapeDtypeStruct((phases, count, slots), f32),
        ),
        in_specs=[vmem()] * 13 + [hbm()] * 4,
        out_specs=(vmem(), vmem()),
        scratch_shapes=[
            pltpu.VMEM(wave.shape, f32),
            pltpu.VMEM(admit.shape, f32),
            pltpu.VMEM(hist.shape, f32),
            pltpu.VMEM((lines, inverse.shape[0], width), bf16),
            pltpu.VMEM((lines, inverse.shape[0], width), bf16),
            pltpu.VMEM((phases, lines, width, slots), bf16),
            pltpu.VMEM((phases, lines, slots, width) if turned else (SUBLANES, LANES), bf16),
            pltpu.VMEM((devices * max(base, SUBLANES), slots), bf16),
            pltpu.VMEM((devices * left, (groups + tiles) * slots), bf16),
            pltpu.VMEM((2 * LANES, (groups + tiles) * slots), bf16),
            pltpu.VMEM((STEPS, phases * phases, slots), f32),
            pltpu.VMEM((STEPS, phases * phases, slots), f32),
            pltpu.VMEM((STEPS, phases, count, slots), f32),
            pltpu.VMEM((phases, count, slots), f32),
            pltpu.VMEM((phases, count, slots), f32),
            pltpu.VMEM((phases, 2 * half, slots), bf16),
            pltpu.VMEM((count, width), f32),
            pltpu.VMEM((lines, count, width), f32),
            pltpu.VMEM((lines, count, width), f32),
            pltpu.VMEM((chips, count, width), f32),
            pltpu.VMEM((chips, count, width), f32),
            pltpu.VMEM((chips, count, width), f32),
            pltpu.VMEM((2, chips, count, width), f32),
            pltpu.VMEM((SPLIT, devices, message, LANES), f32),
            pltpu.VMEM((STEPS - 1, SPLIT, devices, message, LANES), f32),
            dma(3), dma(lines), dma(chips, SPLIT), dma(chips, SPLIT), dma(chips, SPLIT, PIECES), dma(2, chips, SPLIT, PIECES),
        ] + gather_sems + gather_sems + [dma(SPLIT, devices), dma(STEPS - 1, SPLIT, devices)],
        compiler_params=pltpu.CompilerParams(
            collective_id=0, has_side_effects=True, vmem_limit_bytes=67043328
        ),
        name="network",
    )(
        prior, sources, fault_node[None], fault_conductance[None], terminal[:, None], ownership, partner,
        delay_steps, surge_conductance, pole_wave[0][:, None], residue_wave[0][:, :, :, None],
        pole_admit[0][:, None], residue_admit[0][:, :, :, None],
        inverse, wave, admit, hist,
    )
    volt, curr = pl.pallas_call(
        hand_over,
        out_shape=(jax.ShapeDtypeStruct(volt.shape, f32), jax.ShapeDtypeStruct(curr.shape, f32)),
        in_specs=[vmem(), vmem()],
        out_specs=(vmem(), vmem()),
        name="hand_over",
    )(volt, curr)
    return volt[None], curr[None]


def solution(mesh):
    return jax.shard_map(
        on_device,
        mesh=mesh,
        in_specs=(
            P("net", "line", None),
            P("net", None, "line"),
            P(None, "net", "line"),
            P(),
            P(),
            P("net", None, "line"),
            P("net", "line"),
            P("net", "line"),
            P("net", "line"),
            P("net", "line"),
            P("net", None, "line"),
            P("net", None, None, None, "line"),
            P("net", None, "line"),
            P("net", None, None, None, "line"),
            P("net", None, None, None, "line"),
            P("net", None, None, None, "line"),
            P("net", None, None, None, "line"),
        ),
        out_specs=(P("net", None, "line"), P("net", None, None, "line")),
        check_vma=False,
    )
```
